32 devices in a mesh: gx: 8 (over z, y), gy: 4 (over x, core).
Axes of the slice: x: 2, y: 2, z: 4, core: 2. Of those that a mesh axis runs over, the one named last changes fastest.
Arguments:
- liquid_starting_warmth: float32 [32, 64, 1024], P('gx', 'gy'), may hold values from -6 to 6
- liquid_spreading_ratios: float32 [32, 64, 1024], P('gx', 'gy'), may hold values from 0.02 to 0.12
- liquid_advective_ratios: float32 [3, 32, 64, 1024], P(None, 'gx', 'gy'), may hold values from -0.08 to 0.08
- liquid_refresh_flags: int32 [32, 64, 8], P('gx', 'gy'), may hold values 0 or 1
- wall_starting_warmth: float32 [32, 64, 1024], P('gx', 'gy'), may hold values from -6 to 6
- wall_thermal_capacity: float32 [32, 64, 1024], P('gx', 'gy'), may hold values from 0.5 to 2
- thermal_conductance: float32 [32, 64, 1024], P('gx', 'gy'), may hold values from 0.5 to 15
- wall_energy_output: float32 [32, 64, 1024], P('gx', 'gy'), may hold values from -36 to 36
- coupling_partner_lookup: int32 [32, 64], P('gx', 'gy'), may hold values from 0 to 63, each once within a row
Outputs:
- fluid_after: float32 [32, 64, 1024], P('gx', 'gy')
- solid_after: float32 [32, 64, 1024], P('gx', 'gy')
The draws below stay inside these ranges and needn't reach their ends.
Inputs may be any that keep to these rules, and one draw needn't show every extreme that they name: For each first index, the row of coupling_partner_lookup holds every number of 0 to 63 once.
All inputs are finite; a program needn't handle non-finite values. No bound on the sum of `liquid_refresh_flags` on one device may be relied on, other than what follows from the above.
Results may differ from the reference program's by a relative error of at most 0.00023.
Values sent between devices are 32-bit elements; how exact they have to be, the bound alone decides.
A program may use at most 64 MiB of HBM per device.

```python
import math
import jax
import jax.numpy as jnp

VOLUMES_ALONG_Z = 1024
SUBSTEPS = 4
ITERS = 4
ZB = 128
VOLUMES_ALONG_X = 32
VOLUMES_ALONG_Y = 64


def draw_thermal_conductance(key, part):
    baseline = jnp.exp(jax.random.uniform(key, (VOLUMES_ALONG_X, VOLUMES_ALONG_Y, VOLUMES_ALONG_Z), jnp.float32, math.log(0.5), math.log(5.0)))
    ramp_up = 1.0 + 2.0 * jnp.arange(VOLUMES_ALONG_X, dtype=jnp.float32) / (VOLUMES_ALONG_X - 1)
    return baseline * ramp_up[:, None, None]


def draw_wall_energy_output(key, part):
    along_x = 1.0 + 2.0 * jnp.arange(VOLUMES_ALONG_X, dtype=jnp.float32) / (VOLUMES_ALONG_X - 1)
    along_y = 1.0 + 2.0 * jnp.arange(VOLUMES_ALONG_Y, dtype=jnp.float32) / (VOLUMES_ALONG_Y - 1)
    scaling = along_x[:, None, None] * along_y[None, :, None]
    samples = jax.random.truncated_normal(key, -4.0, 4.0, (VOLUMES_ALONG_X, VOLUMES_ALONG_Y, VOLUMES_ALONG_Z), jnp.float32)
    return samples * scaling


def with_ends(entries, rng, least, top_value):
    spot = [jax.random.randint(jax.random.fold_in(rng, axis), (), 0, length) for axis, length in enumerate(entries.shape)]
    widest = entries.shape.index(max(entries.shape))
    beside = spot[:widest] + [(spot[widest] + 1) % entries.shape[widest]] + spot[widest + 1:]
    return entries.at[tuple(spot)].set(least).at[tuple(beside)].set(top_value)


def block_scale(stream_key, dims, cuts, least, largest):
    def one(position, blocks):
        draws = jax.random.uniform(jax.random.fold_in(jax.random.fold_in(stream_key, 6), position), (blocks,), jnp.float32, least / len(cuts), largest / len(cuts))
        return jnp.repeat(jnp.exp(draws), dims[position] // blocks).reshape((-1,) + (1,) * (len(dims) - position - 1))

    gain = one(*cuts[0])
    for cut in cuts[1:]:
        gain = gain * one(*cut)
    return gain


def scatter_about(rng, extent, scale, reach, shards=(), kind=jnp.bfloat16):
    gain = block_scale(rng, extent, shards, -0.22, 0.18) if shards else 1.0
    entries = jax.random.normal(rng, extent, jnp.float32) * scale * gain
    return jnp.minimum(jnp.maximum(entries, -reach), reach).astype(kind)


def setup_inputs(seed: int = 0) -> dict:
    key_list = jax.random.split(jax.random.key(seed), 10)
    return {
        "liquid_starting_warmth": scatter_about(key_list[0], (VOLUMES_ALONG_X, VOLUMES_ALONG_Y, VOLUMES_ALONG_Z), 1.0, 6.0, ((0, 8), (1, 4)), jnp.float32),
        "liquid_spreading_ratios": jnp.clip(jnp.exp(math.log(0.12) - 1.7917595 * jax.random.uniform(key_list[1], (VOLUMES_ALONG_X, VOLUMES_ALONG_Y, VOLUMES_ALONG_Z), jnp.float32) ** block_scale(key_list[1], (VOLUMES_ALONG_X, VOLUMES_ALONG_Y, VOLUMES_ALONG_Z), ((0, 8), (1, 4)), -0.2, 0.2)), 0.02, 0.12),
        "liquid_advective_ratios": jnp.clip(jax.random.uniform(key_list[2], (3, VOLUMES_ALONG_X, VOLUMES_ALONG_Y, VOLUMES_ALONG_Z), jnp.float32, -0.08, 0.08) * block_scale(key_list[2], (3, VOLUMES_ALONG_X, VOLUMES_ALONG_Y, VOLUMES_ALONG_Z), ((1, 8), (2, 4)), -0.4, 0.0), -0.08, 0.08),
        "liquid_refresh_flags": with_ends((jax.random.randint(key_list[3], (VOLUMES_ALONG_X, VOLUMES_ALONG_Y, VOLUMES_ALONG_Z // ZB), 0, 4) < 3).astype(jnp.int32), jax.random.fold_in(key_list[3], 1), 0, 1),
        "wall_starting_warmth": scatter_about(key_list[4], (VOLUMES_ALONG_X, VOLUMES_ALONG_Y, VOLUMES_ALONG_Z), 1.0, 6.0, ((0, 8), (1, 4)), jnp.float32),
        "wall_thermal_capacity": jnp.clip(jnp.exp(math.log(2.0) - 1.3862944 * jax.random.uniform(key_list[5], (VOLUMES_ALONG_X, VOLUMES_ALONG_Y, VOLUMES_ALONG_Z), jnp.float32) ** block_scale(key_list[5], (VOLUMES_ALONG_X, VOLUMES_ALONG_Y, VOLUMES_ALONG_Z), ((0, 8), (1, 4)), -0.2, 0.2)), 0.5, 2.0),
        "thermal_conductance": draw_thermal_conductance(jax.random.fold_in(key_list[9], 71), 0),
        "wall_energy_output": draw_wall_energy_output(jax.random.fold_in(key_list[9], 71), 0),
        "coupling_partner_lookup": jax.vmap(lambda own: jax.random.permutation(own, VOLUMES_ALONG_Y))(jax.random.split(key_list[8], VOLUMES_ALONG_X)).reshape((VOLUMES_ALONG_X, VOLUMES_ALONG_Y)).astype(jnp.int32),
    }


def advance(current_estimate, padded, ghost_row, diffusion, velocity, active_cells):
    below = jnp.concatenate([ghost_row[:, :, None], current_estimate[:, :, :-1]], axis=2)
    above = jnp.concatenate([current_estimate[:, :, 1:], jnp.zeros_like(current_estimate[:, :, :1])], axis=2)
    couples = ((padded[:-2, 1:-1], padded[2:, 1:-1]), (padded[1:-1, :-2], padded[1:-1, 2:]), (below, above))
    spread = -6.0 * current_estimate
    carried = jnp.zeros_like(current_estimate)
    for component in range(3):
        behind, ahead = couples[component]
        spread = spread + behind + ahead
        flow_speed = velocity[component]
        carried = carried + jnp.maximum(flow_speed, 0.0) * (current_estimate - behind) + jnp.minimum(flow_speed, 0.0) * (ahead - current_estimate)
    return current_estimate + active_cells * (diffusion * spread - carried)


def neighbours(field, padded):
    below = jnp.concatenate([jnp.zeros_like(field[:, :, :1]), field[:, :, :-1]], axis=2)
    above = jnp.concatenate([field[:, :, 1:], jnp.zeros_like(field[:, :, :1])], axis=2)
    return (padded[:-2, 1:-1], padded[2:, 1:-1], padded[1:-1, :-2], padded[1:-1, 2:], below, above)


def thermal_flow_operator(field, padded_field, thermal_conductance, bordered_conductance, capacity):
    accumulated = capacity * field
    for near_value, near_cond in zip(neighbours(field, padded_field), neighbours(thermal_conductance, bordered_conductance)):
        accumulated = accumulated + 0.5 * (thermal_conductance + near_cond) * (field - near_value)
    return accumulated


def diagonal_of(thermal_conductance, bordered_conductance, capacity):
    accumulated = capacity
    for near_cond in neighbours(thermal_conductance, bordered_conductance):
        accumulated = accumulated + 0.5 * (thermal_conductance + near_cond)
    return accumulated


def border_margin(field):
    return jnp.pad(field, ((1, 1), (1, 1), (0, 0)))


def reference(liquid_starting_warmth, liquid_spreading_ratios, liquid_advective_ratios, liquid_refresh_flags, wall_starting_warmth, wall_thermal_capacity, thermal_conductance, wall_energy_output, coupling_partner_lookup):
    active_cells = jnp.repeat(liquid_refresh_flags.astype(jnp.float32), ZB, axis=2)
    topmost_layers = wall_starting_warmth[:, :, -1]
    ghost_row = jnp.take_along_axis(topmost_layers, coupling_partner_lookup, axis=1)
    current_estimate = liquid_starting_warmth
    flux_sum = jnp.zeros_like(ghost_row)
    for substep in range(SUBSTEPS):
        flux_sum = flux_sum + (current_estimate[:, :, 0] - ghost_row)
        current_estimate = advance(current_estimate, border_margin(current_estimate), ghost_row, liquid_spreading_ratios, liquid_advective_ratios, active_cells)
    flux_mean = flux_sum / SUBSTEPS
    row_ids = jnp.arange(VOLUMES_ALONG_X, dtype=jnp.int32)[:, None]
    arrived = jnp.zeros_like(flux_mean).at[row_ids, coupling_partner_lookup].add(flux_mean)
    equation_source_term = wall_thermal_capacity * wall_starting_warmth + wall_energy_output
    equation_source_term = equation_source_term.at[:, :, -1].add(arrived)
    bordered_conductance = border_margin(thermal_conductance)
    diagonal = diagonal_of(thermal_conductance, bordered_conductance, wall_thermal_capacity)
    converged_warmth = wall_starting_warmth
    leftover_error = equation_source_term - thermal_flow_operator(converged_warmth, border_margin(converged_warmth), thermal_conductance, bordered_conductance, wall_thermal_capacity)
    scaled = leftover_error / diagonal
    search_heading = scaled
    inner_rz = jnp.sum(leftover_error * scaled)
    for iteration in range(ITERS):
        image = thermal_flow_operator(search_heading, border_margin(search_heading), thermal_conductance, bordered_conductance, wall_thermal_capacity)
        descent_length = inner_rz / jnp.sum(search_heading * image)
        converged_warmth = converged_warmth + descent_length * search_heading
        leftover_error = leftover_error - descent_length * image
        scaled = leftover_error / diagonal
        inner_next = jnp.sum(leftover_error * scaled)
        search_heading = scaled + (inner_next / inner_rz) * search_heading
        inner_rz = inner_next
    return current_estimate, converged_warmth
```

```python
import functools

import jax
import jax.numpy as jnp
from jax import lax
from jax.experimental import pallas as pl
from jax.experimental.pallas import tpu as pltpu
from jax.sharding import PartitionSpec as P

SUBSTEPS = 4
ITERS = 4
ZB = 128
LANES = 128
MESH = pl.DeviceIdType.MESH
F32 = jnp.float32

ST_P = 0
ST_U = ST_P + SUBSTEPS - 1
ST_K = ST_U + SUBSTEPS
ST_V = ST_K + 1
ST_W = ST_V + 1
STAGES = ST_W + ITERS


def kernel(
    nx, ny,
    u_hbm, d_hbm, c_hbm, flags_hbm, v_hbm, cap_hbm, k_hbm, heat_hbm, map_hbm,
    u_out, v_out,
    U, Pb, K, V, W,
    yU, yP, yK, yV, yW,
    sU, sP, sK, sV, sW,
    D, C, FLAGS, CAP, HEAT, MAP,
    CC, CXm, CXp, CYm, CYp, CZm, CZp, Q, GH, LK, FS,
    GX, GYm, GYp, GZm, GZp, DI, INV,
    TG, AG, MU, MGY, MSX, MGX, UO, VO,
    in_sem, out_sem, hs_sem, hr_sem, tg_s, tg_r, ag_s, ag_r, my_s, my_r, mx_s, mx_r,
):
    gx = lax.axis_index("gx")
    gy = lax.axis_index("gy")
    lx, ly, zz = CAP.shape
    wg = TG.shape[-1]

    loads = {}

    def load(name, src, dst, n):
        cp = pltpu.make_async_copy(src, dst, in_sem.at[n])
        cp.start()
        loads[name] = cp

    load("u", u_hbm, U.at[0, pl.ds(1, lx)], 0)
    load("v", v_hbm, V.at[pl.ds(1, lx)], 1)
    load("k", k_hbm, K.at[pl.ds(1, lx)], 2)
    load("map", map_hbm, MAP, 3)
    load("flags", flags_hbm, FLAGS, 4)
    load("d", d_hbm, D, 5)
    load("c", c_hbm, C, 6)
    load("heat", heat_hbm, HEAT, 7)
    load("cap", cap_hbm, CAP, 8)

    barrier = pltpu.get_barrier_semaphore()
    for p in range(1, nx):
        pl.semaphore_signal(barrier, 1, device_id={"gx": lax.rem(gx + p, nx)}, device_id_type=MESH)
    for p in range(1, ny):
        pl.semaphore_signal(barrier, 1, device_id={"gy": lax.rem(gy + p, ny)}, device_id_type=MESH)

    bodies = (
        [(Pb.at[s], yP.at[s]) for s in range(SUBSTEPS - 1)]
        + [(U.at[s], yU.at[s]) for s in range(SUBSTEPS)]
        + [(K, yK), (V, yV)]
        + [(W.at[s], yW.at[s]) for s in range(ITERS)]
    )
    stagings = (
        [sP.at[s] for s in range(SUBSTEPS - 1)]
        + [sU.at[s] for s in range(SUBSTEPS)]
        + [sK, sV]
        + [sW.at[s] for s in range(ITERS)]
    )

    @pl.when(gx == 0)
    def _():
        for body, _y in bodies:
            body[0] = jnp.zeros(body.shape[1:], F32)

    @pl.when(gx == nx - 1)
    def _():
        for body, _y in bodies:
            body[lx + 1] = jnp.zeros(body.shape[1:], F32)

    @pl.when(gy == 0)
    def _():
        for _b, y in bodies:
            y[0] = jnp.zeros(y.shape[1:], F32)

    @pl.when(gy == ny - 1)
    def _():
        for _b, y in bodies:
            y[1] = jnp.zeros(y.shape[1:], F32)

    pl.semaphore_wait(barrier, nx + ny - 2)

    has = (gx > 0, gx < nx - 1, gy > 0, gy < ny - 1)
    to = (
        {"gx": jnp.maximum(gx - 1, 0)},
        {"gx": jnp.minimum(gx + 1, nx - 1)},
        {"gy": jnp.maximum(gy - 1, 0)},
        {"gy": jnp.minimum(gy + 1, ny - 1)},
    )

    def halo_copy(stage, d):
        body, y = bodies[stage]
        stag = stagings[stage]
        src, dst = (
            (body.at[1], body.at[lx + 1]),
            (body.at[lx], body.at[0]),
            (stag.at[0], y.at[1]),
            (stag.at[1], y.at[0]),
        )[d]
        return pltpu.make_async_remote_copy(
            src_ref=src, dst_ref=dst, send_sem=hs_sem.at[stage, d], recv_sem=hr_sem.at[stage, d],
            device_id=to[d], device_id_type=MESH,
        )

    def send(stage):
        for d in (0, 1, 2, 3):
            @pl.when(has[d])
            def _():
                halo_copy(stage, d).start()

    def arrive(stage):
        for d in (0, 1, 2, 3):
            @pl.when(has[d ^ 1])
            def _():
                halo_copy(stage, d).wait_recv()

    def sent(stage):
        for d in (0, 1, 2, 3):
            @pl.when(has[d])
            def _():
                halo_copy(stage, d).wait_send()

    def gather(buf, axis, n, me, ss, rs):
        copies = []
        for p in range(1, n):
            cp = pltpu.make_async_remote_copy(
                src_ref=buf.at[0], dst_ref=buf.at[p], send_sem=ss.at[p], recv_sem=rs.at[p],
                device_id={axis: lax.rem(me + p, n)}, device_id_type=MESH,
            )
            cp.start()
            copies.append(cp)
        return copies

    def rows(fn):
        def step(i, carry):
            fn(i)
            return carry
        lax.fori_loop(0, lx, step, 0)

    def stage_y(stage, i, x):
        stag = stagings[stage]
        stag[0, i] = x[0:1, :]
        stag[1, i] = x[ly - 1:ly, :]

    def sides(body, y, i):
        x = body[i + 1]
        z = x.shape[1]
        sub = lax.broadcasted_iota(jnp.int32, x.shape, 0)
        ym = jnp.where(sub == 0, y[0, i], pltpu.roll(x, 1, 0))
        yp = jnp.where(sub == ly - 1, y[1, i], pltpu.roll(x, ly - 1, 0))
        return x, body[i], body[i + 2], ym, yp, pltpu.roll(x, 1, 1), pltpu.roll(x, z - 1, 1)

    lane_g = lax.broadcasted_iota(jnp.int32, (ly, wg), 1)
    sub_g = lax.broadcasted_iota(jnp.int32, (ly, wg), 0)
    own_g = lane_g == gy * ly + sub_g
    lane_gf = lane_g.astype(F32)
    lane_t = lax.broadcasted_iota(jnp.int32, (ly, LANES), 1)
    lane_z = lax.broadcasted_iota(jnp.int32, (ly, zz), 1)

    loads["u"].wait()

    def take_low(i):
        x = U[0, i + 1, :, 0:LANES]
        Pb[0, i + 1] = x
        stage_y(ST_P, i, x)
    rows(take_low)
    send(ST_P)

    loads["v"].wait()

    def take_top(i):
        last = V[i + 1, :, zz - LANES:zz]
        TG[0, i] = jnp.sum(jnp.where(own_g, last[:, LANES - 1:LANES], 0.0), axis=0, keepdims=True)
        stage_y(ST_V, i, V[i + 1])
        stage_y(ST_U, i, U[0, i + 1])
    rows(take_top)
    tops = gather(TG, "gy", ny, gy, tg_s, tg_r)

    loads["k"].wait()

    def take_k(i):
        stage_y(ST_K, i, K[i + 1])
    rows(take_k)
    send(ST_K)

    loads["map"].wait()
    loads["flags"].wait()
    loads["d"].wait()
    loads["c"].wait()
    eye = lax.broadcasted_iota(jnp.int32, (ly, ly), 0) == lax.broadcasted_iota(jnp.int32, (ly, ly), 1)
    for i in range(lx):
        line = MAP[i:i + 1, :].astype(F32)
        lk = jnp.sum(jnp.where(eye, line, 0.0), axis=1, keepdims=True)
        LK[i] = jnp.broadcast_to(lk, (ly, LANES))

    def fluid_coefficients(i):
        flags = FLAGS[i].astype(F32)
        for t in range(zz // ZB):
            sl = pl.ds(t * ZB, ZB)
            on = jnp.broadcast_to(flags[:, t:t + 1], (ly, ZB))
            spread = on * D[i, :, sl]
            total = None
            for comp, (lo, hi) in enumerate(((CXm, CXp), (CYm, CYp), (CZm, CZp))):
                flow = on * C[comp, i, :, sl]
                a = spread + jnp.maximum(flow, 0.0)
                b = spread - jnp.minimum(flow, 0.0)
                total = a + b if total is None else total + (a + b)
                if comp == 2 and t == 0:
                    lane = lax.broadcasted_iota(jnp.int32, (ly, ZB), 1)
                    Q[i] = jnp.where(lane == 0, a, 0.0)[:, 0:LANES]
                    a = jnp.where(lane == 0, 0.0, a)
                if comp == 2 and t == zz // ZB - 1:
                    lane = lax.broadcasted_iota(jnp.int32, (ly, ZB), 1)
                    b = jnp.where(lane == ZB - 1, 0.0, b)
                lo[i, :, sl] = a
                hi[i, :, sl] = b
            CC[i, :, sl] = 1.0 - total
    rows(fluid_coefficients)

    for cp in tops:
        cp.wait_recv()

    def ghosts(i):
        whole = TG[0, i]
        for p in range(1, ny):
            whole = whole + TG[p, i]
        pick = jnp.where(lane_gf == LK[i, :, 0:1], whole, 0.0)
        ghost = jnp.sum(pick, axis=1, keepdims=True)
        GH[i] = jnp.broadcast_to(ghost, (ly, LANES))
        Q[i] = Q[i] * ghost
        FS[i] = Pb[0, i + 1] - ghost
    rows(ghosts)

    def fluid(body, y, i, z):
        x, a, b, c, d, e, f = sides(body, y, i)
        sl = pl.ds(0, z)
        return (CC[i, :, sl] * x + CXm[i, :, sl] * a + CXp[i, :, sl] * b + CYm[i, :, sl] * c
                + CYp[i, :, sl] * d + CZm[i, :, sl] * e + CZp[i, :, sl] * f)

    for s in range(SUBSTEPS - 1):
        arrive(ST_P + s)

        def low(i):
            new = fluid(Pb.at[s], yP.at[s], i, LANES) + Q[i]
            FS[i] = FS[i] + (new - GH[i])
            if s + 1 < SUBSTEPS - 1:
                Pb[s + 1, i + 1] = new
                stage_y(ST_P + s + 1, i, new)
        rows(low)
        if s + 1 < SUBSTEPS - 1:
            send(ST_P + s + 1)
        if s == 0:
            send(ST_V)

    def scatter(i):
        mean = FS[i][:, 0:1] * (1.0 / SUBSTEPS)
        AG[0, i] = jnp.sum(jnp.where(lane_gf == LK[i, :, 0:1], mean, 0.0), axis=0, keepdims=True)
    rows(scatter)
    fluxes = gather(AG, "gy", ny, gy, ag_s, ag_r)
    send(ST_U)

    arrive(ST_K)
    loads["cap"].wait()
    loads["heat"].wait()
    for f in range(lx + 1):
        GX[f] = 0.5 * (K[f] + K[f + 1])

    def solid_coefficients(i):
        k, _a, _b, c, d, e, f = sides(K, yK, i)
        gxm, gxp, gym, gyp = GX[i], GX[i + 1], 0.5 * (k + c), 0.5 * (k + d)
        gzm = 0.5 * (k + jnp.where(lane_z == 0, 0.0, e))
        gzp = 0.5 * (k + jnp.where(lane_z == zz - 1, 0.0, f))
        diag = CAP[i] + (gxm + gxp + gym + gyp + gzm + gzp)
        DI[i] = diag
        INV[i] = 1.0 / diag
        GYm[i] = gym
        GYp[i] = gyp
        GZm[i] = jnp.where(lane_z == 0, 0.0, gzm)
        GZp[i] = jnp.where(lane_z == zz - 1, 0.0, gzp)
    rows(solid_coefficients)

    def pull(body, y, i):
        x, a, b, c, d, e, f = sides(body, y, i)
        return x, (GX[i] * a + GX[i + 1] * b + GYm[i] * c + GYp[i] * d + GZm[i] * e + GZp[i] * f)

    arrive(ST_V)

    def first(i):
        x, s = pull(V, yV, i)
        W[0, i + 1] = (HEAT[i] - (DI[i] - CAP[i]) * x + s) * INV[i]
    rows(first)

    for cp in fluxes:
        cp.wait_recv()

    def fold(x):
        acc = x[0:8, 0:LANES]
        for r in range(0, ly, 8):
            for t in range(0, zz, LANES):
                if r or t:
                    acc = acc + x[r:r + 8, t:t + LANES]
        return jnp.sum(acc, axis=0, keepdims=True)

    def add_flux(i):
        whole = AG[0, i]
        for p in range(1, ny):
            whole = whole + AG[p, i]
        got = jnp.sum(jnp.where(own_g, whole, 0.0), axis=1, keepdims=True)
        sl = pl.ds(zz - LANES, LANES)
        W[0, i + 1, :, sl] = W[0, i + 1, :, sl] + jnp.where(lane_t == LANES - 1, got, 0.0) * INV[i, :, sl]
        stage_y(ST_W, i, W[0, i + 1])
    rows(add_flux)
    send(ST_W)

    MU[...] = jnp.zeros(MU.shape, F32)

    def norm(i):
        w = W[0, i + 1]
        MU[0:1] = MU[0:1] + fold(w * w * DI[i])
    rows(norm)

    for s in range(max(SUBSTEPS, ITERS)):
        if s < SUBSTEPS:
            arrive(ST_U + s)
            last_u = s + 1 == SUBSTEPS

            def bulk(i):
                new = fluid(U.at[s], yU.at[s], i, zz)
                head = new[:, 0:LANES] + Q[i]
                if last_u:
                    UO[i] = new
                    UO[i, :, 0:LANES] = head
                else:
                    U[s + 1, i + 1] = new
                    U[s + 1, i + 1, :, 0:LANES] = head
                    stage_y(ST_U + s + 1, i, U[s + 1, i + 1])
            rows(bulk)
            if last_u:
                out_u = pltpu.make_async_copy(UO, u_out, out_sem.at[0])
                out_u.start()
            else:
                send(ST_U + s + 1)
        if s < ITERS:
            arrive(ST_W + s)
            last_w = s + 1 == ITERS

            def apply(i):
                x, pulled = pull(W.at[s], yW.at[s], i)
                MU[2 * s + 1:2 * s + 2] = MU[2 * s + 1:2 * s + 2] + fold(x * pulled)
                if not last_w:
                    new = pulled * INV[i]
                    W[s + 1, i + 1] = new
                    stage_y(ST_W + s + 1, i, new)
                    MU[2 * s + 2:2 * s + 3] = MU[2 * s + 2:2 * s + 3] + fold(new * pulled)
            rows(apply)
            if not last_w:
                send(ST_W + s + 1)

    MGY[0] = MU[...]
    sums_y = gather(MGY, "gy", ny, gy, my_s, my_r)
    for cp in sums_y:
        cp.wait_recv()
    total = MGY[0]
    for p in range(1, ny):
        total = total + MGY[p]
    MGX[0] = jnp.broadcast_to(jnp.sum(total, axis=1, keepdims=True), total.shape)
    sums_x = gather(MGX, "gx", nx, gx, mx_s, mx_r)
    for cp in sums_x:
        cp.wait_recv()


    total = jnp.zeros(MU.shape, F32)
    for p in range(nx):
        total = total + MGX[p]
    mu = [total[m:m + 1, :] for m in range(2 * ITERS)]

    tiny = 1e-30
    G = [[mu[i + j] - mu[i + j + 1] for j in range(ITERS)] for i in range(ITERS)]
    b = [mu[i] for i in range(ITERS)]
    low_f = {}
    rec = []
    for i in range(ITERS):
        good = G[i][i] > jnp.maximum(1e-7 * (mu[2 * i] + jnp.abs(mu[2 * i + 1])), tiny)
        r = jnp.where(good, 1.0 / jnp.where(good, G[i][i], 1.0), 0.0)
        rec.append(r)
        for j in range(i + 1, ITERS):
            low_f[j, i] = G[j][i] * r
        for j in range(i + 1, ITERS):
            b[j] = b[j] - low_f[j, i] * b[i]
            for m in range(i + 1, ITERS):
                G[j][m] = G[j][m] - low_f[j, i] * G[i][m]
    y = [None] * ITERS
    for i in reversed(range(ITERS)):
        y[i] = b[i] * rec[i]
        for j in range(i + 1, ITERS):
            y[i] = y[i] - low_f[j, i] * y[j]

    ys = [v[:, 0:1] for v in y]

    def finish(i):
        acc = V[i + 1]
        for j in range(ITERS):
            acc = acc + ys[j] * W[j, i + 1]
        VO[i] = acc
    rows(finish)
    out_v = pltpu.make_async_copy(VO, v_out, out_sem.at[1])
    out_v.start()

    for stage in range(STAGES):
        sent(stage)
    for cp in tops + fluxes + sums_y + sums_x:
        cp.wait_send()
    out_u.wait()
    out_v.wait()


def solution(mesh):
    nx, ny = mesh.shape["gx"], mesh.shape["gy"]

    def local(u, d, c, flags, v, cap, k, heat, lookup):
        lx, ly, zz = u.shape
        wg = -(-(ny * ly) // LANES) * LANES
        field = (lx, ly, zz)
        padded = (lx + 2, ly, zz)
        edge = (2, lx, 1, zz)
        low = (2, lx, 1, LANES)
        tile = (lx, ly, LANES)
        vm = lambda *shape: pltpu.VMEM(shape, F32)
        ns = SUBSTEPS
        scratch = [
            vm(ns, *padded), vm(ns - 1, lx + 2, ly, LANES), vm(*padded), vm(*padded), vm(ITERS, *padded),
            vm(ns, *edge), vm(ns - 1, *low), vm(*edge), vm(*edge), vm(ITERS, *edge),
            vm(ns, *edge), vm(ns - 1, *low), vm(*edge), vm(*edge), vm(ITERS, *edge),
            vm(*field), vm(3, *field), pltpu.VMEM(flags.shape, jnp.int32), vm(*field), vm(*field),
            pltpu.VMEM(lookup.shape, jnp.int32),
        ]
        scratch += [vm(*field)] * 7 + [vm(*tile)] * 4
        scratch += [vm(lx + 1, ly, zz)] + [vm(*field)] * 6
        scratch += [
            vm(ny, lx, 1, wg), vm(ny, lx, 1, wg), vm(2 * ITERS, LANES), vm(ny, 2 * ITERS, LANES),
            vm(2 * ITERS, LANES), vm(nx, 2 * ITERS, LANES), vm(*field), vm(*field),
        ]
        dma = lambda *shape: pltpu.SemaphoreType.DMA(shape)
        scratch += [
            dma(9), dma(2), dma(STAGES, 4), dma(STAGES, 4),
            dma(ny), dma(ny), dma(ny), dma(ny), dma(ny), dma(ny), dma(nx), dma(nx),
        ]
        return pl.pallas_call(
            functools.partial(kernel, nx, ny),
            out_shape=(jax.ShapeDtypeStruct(field, F32),) * 2,
            in_specs=[pl.BlockSpec(memory_space=pl.ANY)] * 9,
            out_specs=(pl.BlockSpec(memory_space=pl.ANY),) * 2,
            scratch_shapes=scratch,
            compiler_params=pltpu.CompilerParams(
                collective_id=0, has_side_effects=True, vmem_limit_bytes=40 * 1024 * 1024
            ),
        )(u, d, c, flags, v, cap, k, heat, lookup)

    s3 = P("gx", "gy", None)
    return jax.shard_map(
        local,
        mesh=mesh,
        in_specs=(s3, s3, P(None, "gx", "gy", None), s3, s3, s3, s3, s3, P("gx", "gy")),
        out_specs=(s3, s3),
        check_vma=False,
    )
```

```python
import functools

import jax
import jax.numpy as jnp
from jax import lax
from jax.experimental import pallas as pl
from jax.experimental.pallas import tpu as pltpu
from jax.sharding import PartitionSpec as P

SUBSTEPS = 4
ITERS = 4
ZB = 128
LANES = 128
MESH = pl.DeviceIdType.MESH
F32 = jnp.float32

ST_P = 0
ST_U = ST_P + SUBSTEPS - 1
ST_K = ST_U + SUBSTEPS
ST_V = ST_K + 1
ST_W = ST_V + 1
STAGES = ST_W + ITERS


def kernel(
    nx, ny,
    u_hbm, d_hbm, c_hbm, flags_hbm, v_hbm, cap_hbm, k_hbm, heat_hbm, map_hbm,
    u_out, v_out,
    U, Pb, K, V, W,
    yU, yP, yK, yV, yW,
    sU, sP, sK, sV, sW,
    D, C, FLAGS, CAP, HEAT, MAP,
    CC, CXm, CXp, CYm, CYp, CZm, CZp, Q, GH, LK, FS,
    GX, GYm, GYp, GZm, GZp, DI, INV,
    TG, AG, MU, MGY, MSX, MGX, UO, VO,
    in_sem, out_sem, hs_sem, hr_sem, tg_s, tg_r, ag_s, ag_r, my_s, my_r, mx_s, mx_r,
):
    gx = lax.axis_index("gx")
    gy = lax.axis_index("gy")
    lx, ly, zz = CAP.shape
    wg = TG.shape[-1]

    loads = {}

    def load(name, src, dst, n):
        cp = pltpu.make_async_copy(src, dst, in_sem.at[n])
        cp.start()
        loads[name] = cp

    load("u", u_hbm, U.at[0, pl.ds(1, lx)], 0)
    load("v", v_hbm, V.at[pl.ds(1, lx)], 1)
    load("k", k_hbm, K.at[pl.ds(1, lx)], 2)
    load("map", map_hbm, MAP, 3)
    load("flags", flags_hbm, FLAGS, 4)
    load("d", d_hbm, D, 5)
    load("c", c_hbm, C, 6)
    load("heat", heat_hbm, HEAT, 7)
    load("cap", cap_hbm, CAP, 8)

    barrier = pltpu.get_barrier_semaphore()
    for p in range(1, nx):
        pl.semaphore_signal(barrier, 1, device_id={"gx": lax.rem(gx + p, nx)}, device_id_type=MESH)
    for p in range(1, ny):
        pl.semaphore_signal(barrier, 1, device_id={"gy": lax.rem(gy + p, ny)}, device_id_type=MESH)

    bodies = (
        [(Pb.at[s], yP.at[s]) for s in range(SUBSTEPS - 1)]
        + [(U.at[s], yU.at[s]) for s in range(SUBSTEPS)]
        + [(K, yK), (V, yV)]
        + [(W.at[s], yW.at[s]) for s in range(ITERS)]
    )
    stagings = (
        [sP.at[s] for s in range(SUBSTEPS - 1)]
        + [sU.at[s] for s in range(SUBSTEPS)]
        + [sK, sV]
        + [sW.at[s] for s in range(ITERS)]
    )

    @pl.when(gx == 0)
    def _():
        for body, _y in bodies:
            body[0] = jnp.zeros(body.shape[1:], F32)

    @pl.when(gx == nx - 1)
    def _():
        for body, _y in bodies:
            body[lx + 1] = jnp.zeros(body.shape[1:], F32)

    @pl.when(gy == 0)
    def _():
        for _b, y in bodies:
            y[0] = jnp.zeros(y.shape[1:], F32)

    @pl.when(gy == ny - 1)
    def _():
        for _b, y in bodies:
            y[1] = jnp.zeros(y.shape[1:], F32)

    W[ITERS - 1, lx + 1] = jnp.zeros((ly, zz), F32)

    pl.semaphore_wait(barrier, nx + ny - 2)

    has = (gx > 0, gx < nx - 1, gy > 0, gy < ny - 1)
    to = (
        {"gx": jnp.maximum(gx - 1, 0)},
        {"gx": jnp.minimum(gx + 1, nx - 1)},
        {"gy": jnp.maximum(gy - 1, 0)},
        {"gy": jnp.minimum(gy + 1, ny - 1)},
    )

    def halo_copy(stage, d):
        body, y = bodies[stage]
        stag = stagings[stage]
        src, dst = (
            (body.at[1], body.at[lx + 1]),
            (body.at[lx], body.at[0]),
            (stag.at[0], y.at[1]),
            (stag.at[1], y.at[0]),
        )[d]
        return pltpu.make_async_remote_copy(
            src_ref=src, dst_ref=dst, send_sem=hs_sem.at[stage, d], recv_sem=hr_sem.at[stage, d],
            device_id=to[d], device_id_type=MESH,
        )

    one_way = ST_W + ITERS - 1

    def dirs(stage, among=(0, 1, 2, 3)):
        return [d for d in among if stage != one_way or d in (1, 3)]

    def send(stage, among=(0, 1, 2, 3)):
        for d in dirs(stage, among):
            @pl.when(has[d])
            def _():
                halo_copy(stage, d).start()

    def arrive(stage):
        for d in dirs(stage):
            @pl.when(has[d ^ 1])
            def _():
                halo_copy(stage, d).wait_recv()

    def sent(stage):
        for d in dirs(stage):
            @pl.when(has[d])
            def _():
                halo_copy(stage, d).wait_send()

    def gather(buf, axis, n, me, ss, rs):
        copies = []
        for p in range(1, n):
            cp = pltpu.make_async_remote_copy(
                src_ref=buf.at[0], dst_ref=buf.at[p], send_sem=ss.at[p], recv_sem=rs.at[p],
                device_id={axis: lax.rem(me + p, n)}, device_id_type=MESH,
            )
            cp.start()
            copies.append(cp)
        return copies

    def rows(fn, stage=None):
        def step(t, carry):
            fn(lax.rem(lx - t, lx))
            if stage is not None:
                @pl.when(t == min(1, lx - 1))
                def _():
                    send(stage, (0, 1))
            return carry
        lax.fori_loop(0, lx, step, 0)
        if stage is not None:
            send(stage, (2, 3))

    def stage_y(stage, i, x):
        stag = stagings[stage]
        stag[0, i] = x[0:1, :]
        stag[1, i] = x[ly - 1:ly, :]

    def sides(body, y, i):
        x = body[i + 1]
        z = x.shape[1]
        sub = lax.broadcasted_iota(jnp.int32, x.shape, 0)
        ym = jnp.where(sub == 0, y[0, i], pltpu.roll(x, 1, 0))
        yp = jnp.where(sub == ly - 1, y[1, i], pltpu.roll(x, ly - 1, 0))
        return x, body[i], body[i + 2], ym, yp, pltpu.roll(x, 1, 1), pltpu.roll(x, z - 1, 1)

    lane_g = lax.broadcasted_iota(jnp.int32, (ly, wg), 1)
    sub_g = lax.broadcasted_iota(jnp.int32, (ly, wg), 0)
    own_g = lane_g == gy * ly + sub_g
    lane_gf = lane_g.astype(F32)
    lane_t = lax.broadcasted_iota(jnp.int32, (ly, LANES), 1)
    lane_z = lax.broadcasted_iota(jnp.int32, (ly, zz), 1)

    loads["u"].wait()

    def take_low(i):
        x = U[0, i + 1, :, 0:LANES]
        Pb[0, i + 1] = x
        stage_y(ST_P, i, x)
    rows(take_low, ST_P)

    loads["v"].wait()

    def take_top(i):
        last = V[i + 1, :, zz - LANES:zz]
        TG[0, i] = jnp.sum(jnp.where(own_g, last[:, LANES - 1:LANES], 0.0), axis=0, keepdims=True)
        stage_y(ST_V, i, V[i + 1])
        stage_y(ST_U, i, U[0, i + 1])
    rows(take_top)
    tops = gather(TG, "gy", ny, gy, tg_s, tg_r)

    loads["k"].wait()

    def take_k(i):
        stage_y(ST_K, i, K[i + 1])
    rows(take_k, ST_K)

    loads["map"].wait()
    loads["flags"].wait()
    loads["d"].wait()
    loads["c"].wait()
    eye = lax.broadcasted_iota(jnp.int32, (ly, ly), 0) == lax.broadcasted_iota(jnp.int32, (ly, ly), 1)
    for i in range(lx):
        line = MAP[i:i + 1, :].astype(F32)
        lk = jnp.sum(jnp.where(eye, line, 0.0), axis=1, keepdims=True)
        LK[i] = jnp.broadcast_to(lk, (ly, LANES))

    def fluid_coefficients(i):
        for t in range(zz // ZB):
            sl = pl.ds(t * ZB, ZB)
            line = FLAGS[i, t:t + 1, :].astype(F32)
            on = jnp.broadcast_to(jnp.sum(jnp.where(eye, line, 0.0), axis=1, keepdims=True), (ly, ZB))
            spread = on * D[i, :, sl]
            total = None
            for comp, (lo, hi) in enumerate(((CXm, CXp), (CYm, CYp), (CZm, CZp))):
                flow = on * C[comp, i, :, sl]
                a = spread + jnp.maximum(flow, 0.0)
                b = spread - jnp.minimum(flow, 0.0)
                total = a + b if total is None else total + (a + b)
                if comp == 2 and t == 0:
                    lane = lax.broadcasted_iota(jnp.int32, (ly, ZB), 1)
                    Q[i] = jnp.where(lane == 0, a, 0.0)[:, 0:LANES]
                    a = jnp.where(lane == 0, 0.0, a)
                if comp == 2 and t == zz // ZB - 1:
                    lane = lax.broadcasted_iota(jnp.int32, (ly, ZB), 1)
                    b = jnp.where(lane == ZB - 1, 0.0, b)
                lo[i, :, sl] = a
                hi[i, :, sl] = b
            CC[i, :, sl] = 1.0 - total
    rows(fluid_coefficients)

    for cp in tops:
        cp.wait_recv()

    def ghosts(i):
        whole = TG[0, i]
        for p in range(1, ny):
            whole = whole + TG[p, i]
        pick = jnp.where(lane_gf == LK[i, :, 0:1], whole, 0.0)
        ghost = jnp.sum(pick, axis=1, keepdims=True)
        GH[i] = jnp.broadcast_to(ghost, (ly, LANES))
        Q[i] = Q[i] * ghost
        FS[i] = Pb[0, i + 1] - ghost
    rows(ghosts)

    def fluid(body, y, i, z):
        x, a, b, c, d, e, f = sides(body, y, i)
        sl = pl.ds(0, z)
        return (CC[i, :, sl] * x + CXm[i, :, sl] * a + CXp[i, :, sl] * b + CYm[i, :, sl] * c
                + CYp[i, :, sl] * d + CZm[i, :, sl] * e + CZp[i, :, sl] * f)

    for s in range(SUBSTEPS - 1):
        arrive(ST_P + s)

        def low(i):
            new = fluid(Pb.at[s], yP.at[s], i, LANES) + Q[i]
            FS[i] = FS[i] + (new - GH[i])
            if s + 1 < SUBSTEPS - 1:
                Pb[s + 1, i + 1] = new
                stage_y(ST_P + s + 1, i, new)
        rows(low, ST_P + s + 1 if s + 1 < SUBSTEPS - 1 else None)
        if s == 0:
            send(ST_V)

    def scatter(i):
        mean = FS[i][:, 0:1] * (1.0 / SUBSTEPS)
        AG[0, i] = jnp.sum(jnp.where(lane_gf == LK[i, :, 0:1], mean, 0.0), axis=0, keepdims=True)
    rows(scatter)
    fluxes = gather(AG, "gy", ny, gy, ag_s, ag_r)
    send(ST_U)

    arrive(ST_K)
    loads["cap"].wait()
    loads["heat"].wait()
    for f in range(lx + 1):
        GX[f] = 0.5 * (K[f] + K[f + 1])

    def solid_coefficients(i):
        k, _a, _b, c, d, e, f = sides(K, yK, i)
        gxm, gxp, gym, gyp = GX[i], GX[i + 1], 0.5 * (k + c), 0.5 * (k + d)
        gzm = 0.5 * (k + jnp.where(lane_z == 0, 0.0, e))
        gzp = 0.5 * (k + jnp.where(lane_z == zz - 1, 0.0, f))
        diag = CAP[i] + (gxm + gxp + gym + gyp + gzm + gzp)
        DI[i] = diag
        INV[i] = 1.0 / diag
        GYm[i] = gym
        GYp[i] = gyp
        GZm[i] = jnp.where(lane_z == 0, 0.0, gzm)
        GZp[i] = jnp.where(lane_z == zz - 1, 0.0, gzp)
    rows(solid_coefficients)

    def pull(body, y, i):
        x, a, b, c, d, e, f = sides(body, y, i)
        return x, (GX[i] * a + GX[i + 1] * b + GYm[i] * c + GYp[i] * d + GZm[i] * e + GZp[i] * f)

    arrive(ST_V)

    def first(i):
        x, s = pull(V, yV, i)
        W[0, i + 1] = (HEAT[i] - (DI[i] - CAP[i]) * x + s) * INV[i]
    rows(first)

    for cp in fluxes:
        cp.wait_recv()

    def fold(x):
        acc = x[0:8, 0:LANES]
        for r in range(0, ly, 8):
            for t in range(0, zz, LANES):
                if r or t:
                    acc = acc + x[r:r + 8, t:t + LANES]
        return jnp.sum(acc, axis=0, keepdims=True)

    def add_flux(i):
        whole = AG[0, i]
        for p in range(1, ny):
            whole = whole + AG[p, i]
        got = jnp.sum(jnp.where(own_g, whole, 0.0), axis=1, keepdims=True)
        sl = pl.ds(zz - LANES, LANES)
        W[0, i + 1, :, sl] = W[0, i + 1, :, sl] + jnp.where(lane_t == LANES - 1, got, 0.0) * INV[i, :, sl]
        stage_y(ST_W, i, W[0, i + 1])
    rows(add_flux, ST_W)

    MU[...] = jnp.zeros(MU.shape, F32)

    def norm(i):
        w = W[0, i + 1]
        MU[0:1] = MU[0:1] + fold(w * w * DI[i])
    rows(norm)

    def fluid_step(s):
        arrive(ST_U + s)
        last_u = s + 1 == SUBSTEPS

        def bulk(i):
            new = fluid(U.at[s], yU.at[s], i, zz)
            head = new[:, 0:LANES] + Q[i]
            if last_u:
                UO[i] = new
                UO[i, :, 0:LANES] = head
            else:
                U[s + 1, i + 1] = new
                U[s + 1, i + 1, :, 0:LANES] = head
                stage_y(ST_U + s + 1, i, U[s + 1, i + 1])
        rows(bulk, None if last_u else ST_U + s + 1)

    def solid_step(s):
        arrive(ST_W + s)

        def apply(i):
            x, pulled = pull(W.at[s], yW.at[s], i)
            MU[2 * s + 1:2 * s + 2] = MU[2 * s + 1:2 * s + 2] + fold(x * pulled)
            new = pulled * INV[i]
            W[s + 1, i + 1] = new
            stage_y(ST_W + s + 1, i, new)
            MU[2 * s + 2:2 * s + 3] = MU[2 * s + 2:2 * s + 3] + fold(new * pulled)
        rows(apply, ST_W + s + 1)

    for s in range(max(SUBSTEPS, ITERS) - 1):
        if s < ITERS - 1:
            solid_step(s)
        if s < SUBSTEPS - 1:
            fluid_step(s)

    arrive(one_way)
    end = ITERS - 1

    def last_moment(i):
        x = W[end, i + 1]
        z = x.shape[1]
        sub = lax.broadcasted_iota(jnp.int32, x.shape, 0)
        twice = jnp.where(i == 0, 2.0, 1.0).astype(F32)
        ym = jnp.where(sub == 0, 2.0 * yW[end, 0, i], pltpu.roll(x, 1, 0))
        yp = jnp.where(sub == ly - 1, 0.0, pltpu.roll(x, ly - 1, 0))
        pulled = (GX[i] * (twice * W[end, i]) + GX[i + 1] * W[end, i + 2] + GYm[i] * ym + GYp[i] * yp
                  + GZm[i] * pltpu.roll(x, 1, 1) + GZp[i] * pltpu.roll(x, z - 1, 1))
        MU[2 * end + 1:2 * end + 2] = MU[2 * end + 1:2 * end + 2] + fold(x * pulled)
    rows(last_moment)

    MGY[0] = MU[...]
    sums_y = gather(MGY, "gy", ny, gy, my_s, my_r)
    for cp in sums_y:
        cp.wait_recv()
    total = MGY[0]
    for p in range(1, ny):
        total = total + MGY[p]
    MGX[0] = jnp.broadcast_to(jnp.sum(total, axis=1, keepdims=True), total.shape)
    sums_x = gather(MGX, "gx", nx, gx, mx_s, mx_r)
    fluid_step(SUBSTEPS - 1)
    out_u = pltpu.make_async_copy(UO, u_out, out_sem.at[0])
    out_u.start()
    for cp in sums_x:
        cp.wait_recv()
    total = MGX[0]
    for p in range(1, nx):
        total = total + MGX[p]
    mu = [total[m:m + 1, :] for m in range(2 * ITERS)]

    tiny = 1e-30
    G = [[mu[i + j] - mu[i + j + 1] for j in range(ITERS)] for i in range(ITERS)]
    b = [mu[i] for i in range(ITERS)]
    low_f = {}
    rec = []
    for i in range(ITERS):
        good = G[i][i] > jnp.maximum(1e-7 * (mu[2 * i] + jnp.abs(mu[2 * i + 1])), tiny)
        r = jnp.where(good, 1.0 / jnp.where(good, G[i][i], 1.0), 0.0)
        rec.append(r)
        for j in range(i + 1, ITERS):
            low_f[j, i] = G[j][i] * r
        for j in range(i + 1, ITERS):
            b[j] = b[j] - low_f[j, i] * b[i]
            for m in range(i + 1, ITERS):
                G[j][m] = G[j][m] - low_f[j, i] * G[i][m]
    y = [None] * ITERS
    for i in reversed(range(ITERS)):
        y[i] = b[i] * rec[i]
        for j in range(i + 1, ITERS):
            y[i] = y[i] - low_f[j, i] * y[j]

    ys = [v[:, 0:1] for v in y]

    def finish(i):
        acc = V[i + 1]
        for j in range(ITERS):
            acc = acc + ys[j] * W[j, i + 1]
        VO[i] = acc
    rows(finish)
    out_v = pltpu.make_async_copy(VO, v_out, out_sem.at[1])
    out_v.start()

    for stage in range(STAGES):
        sent(stage)
    for cp in tops + fluxes + sums_y + sums_x:
        cp.wait_send()
    out_u.wait()
    out_v.wait()


def solution(mesh):
    nx, ny = mesh.shape["gx"], mesh.shape["gy"]

    def local(u, d, c, flags, v, cap, k, heat, lookup):
        lx, ly, zz = u.shape
        wg = -(-(ny * ly) // LANES) * LANES
        field = (lx, ly, zz)
        padded = (lx + 2, ly, zz)
        edge = (2, lx, 1, zz)
        low = (2, lx, 1, LANES)
        tile = (lx, ly, LANES)
        vm = lambda *shape: pltpu.VMEM(shape, F32)
        ns = SUBSTEPS
        scratch = [
            vm(ns, *padded), vm(ns - 1, lx + 2, ly, LANES), vm(*padded), vm(*padded), vm(ITERS, *padded),
            vm(ns, *edge), vm(ns - 1, *low), vm(*edge), vm(*edge), vm(ITERS, *edge),
            vm(ns, *edge), vm(ns - 1, *low), vm(*edge), vm(*edge), vm(ITERS, *edge),
            vm(*field), vm(3, *field), pltpu.VMEM((lx, flags.shape[2], ly), jnp.int32), vm(*field), vm(*field),
            pltpu.VMEM(lookup.shape, jnp.int32),
        ]
        scratch += [vm(*field)] * 7 + [vm(*tile)] * 4
        scratch += [vm(lx + 1, ly, zz)] + [vm(*field)] * 6
        scratch += [
            vm(ny, lx, 1, wg), vm(ny, lx, 1, wg), vm(2 * ITERS, LANES), vm(ny, 2 * ITERS, LANES),
            vm(2 * ITERS, LANES), vm(nx, 2 * ITERS, LANES), vm(*field), vm(*field),
        ]
        dma = lambda *shape: pltpu.SemaphoreType.DMA(shape)
        scratch += [
            dma(9), dma(2), dma(STAGES, 4), dma(STAGES, 4),
            dma(ny), dma(ny), dma(ny), dma(ny), dma(ny), dma(ny), dma(nx), dma(nx),
        ]
        return pl.pallas_call(
            functools.partial(kernel, nx, ny),
            out_shape=(jax.ShapeDtypeStruct(field, F32),) * 2,
            in_specs=[pl.BlockSpec(memory_space=pltpu.HBM)] * 9,
            out_specs=(pl.BlockSpec(memory_space=pl.ANY),) * 2,
            scratch_shapes=scratch,
            compiler_params=pltpu.CompilerParams(
                collective_id=0, has_side_effects=True, vmem_limit_bytes=67_000_000
            ),
        )(u, d, c, jnp.swapaxes(flags, 1, 2), v, cap, k, heat, lookup)

    s3 = P("gx", "gy", None)
    return jax.shard_map(
        local,
        mesh=mesh,
        in_specs=(s3, s3, P(None, "gx", "gy", None), s3, s3, s3, s3, s3, P("gx", "gy")),
        out_specs=(s3, s3),
        check_vma=False,
    )
```

```python
import functools

import jax
import jax.numpy as jnp
from jax import lax
from jax.experimental import pallas as pl
from jax.experimental.pallas import tpu as pltpu
from jax.sharding import PartitionSpec as P

SUBSTEPS = 4
ITERS = 4
ZB = 128
LANES = 128
MESH = pl.DeviceIdType.MESH
F32 = jnp.float32

ST_P = 0
ST_U = ST_P + SUBSTEPS - 1
ST_K = ST_U + SUBSTEPS
ST_V = ST_K + 1
ST_W = ST_V + 1
STAGES = ST_W + ITERS
REACH = 1 + (SUBSTEPS - 1) + (ITERS - 1)


def kernel(
    nx, ny,
    u_hbm, d_hbm, c_hbm, flags_hbm, v_hbm, cap_hbm, k_hbm, heat_hbm, map_hbm,
    u_out, v_out,
    U, Pb, K, V, W,
    yU, yP, yK, yV, yW,
    sU, sP, sK, sV, sW,
    D, C, FLAGS, CAP, HEAT, MAP,
    CC, CXm, CXp, CYm, CYp, CZm, CZp, Q, GH, LK, FS,
    GX, GYm, GYp, GZm, GZp, DI, INV,
    TG, AG, MU, MGY, MSX, MGX, UO, VO,
    in_sem, out_sem, hs_sem, hr_sem, tg_s, tg_r, ag_s, ag_r, my_s, my_r, mx_s, mx_r,
):
    gx = lax.axis_index("gx")
    gy = lax.axis_index("gy")
    lx, ly, zz = CAP.shape
    wg = TG.shape[-1]

    loads = {}

    def load(name, src, dst, n):
        cp = pltpu.make_async_copy(src, dst, in_sem.at[n])
        cp.start()
        loads[name] = cp

    load("u", u_hbm, U.at[0, pl.ds(1, lx)], 0)
    load("v", v_hbm, V.at[pl.ds(1, lx)], 1)
    load("k", k_hbm, K.at[pl.ds(1, lx)], 2)
    load("map", map_hbm, MAP, 3)
    load("flags", flags_hbm, FLAGS, 4)
    load("d", d_hbm, D, 5)
    load("c", c_hbm, C, 6)
    load("heat", heat_hbm, HEAT, 7)
    load("cap", cap_hbm, CAP, 8)

    barrier = pltpu.get_barrier_semaphore()
    near = nx - 1 <= REACH
    if near:
        @pl.when(gx > 0)
        def _():
            pl.semaphore_signal(barrier, 1, device_id={"gx": jnp.maximum(gx - 1, 0)}, device_id_type=MESH)

        @pl.when(gx < nx - 1)
        def _():
            pl.semaphore_signal(barrier, 1, device_id={"gx": jnp.minimum(gx + 1, nx - 1)}, device_id_type=MESH)
    else:
        for p in range(1, nx):
            pl.semaphore_signal(barrier, 1, device_id={"gx": lax.rem(gx + p, nx)}, device_id_type=MESH)
    for p in range(1, ny):
        pl.semaphore_signal(barrier, 1, device_id={"gy": lax.rem(gy + p, ny)}, device_id_type=MESH)

    bodies = (
        [(Pb.at[s], yP.at[s]) for s in range(SUBSTEPS - 1)]
        + [(U.at[s], yU.at[s]) for s in range(SUBSTEPS)]
        + [(K, yK), (V, yV)]
        + [(W.at[s], yW.at[s]) for s in range(ITERS)]
    )
    stagings = (
        [sP.at[s] for s in range(SUBSTEPS - 1)]
        + [sU.at[s] for s in range(SUBSTEPS)]
        + [sK, sV]
        + [sW.at[s] for s in range(ITERS)]
    )

    @pl.when(gx == 0)
    def _():
        for body, _y in bodies:
            body[0] = jnp.zeros(body.shape[1:], F32)

    @pl.when(gx == nx - 1)
    def _():
        for body, _y in bodies:
            body[lx + 1] = jnp.zeros(body.shape[1:], F32)

    @pl.when(gy == 0)
    def _():
        for _b, y in bodies:
            y[0] = jnp.zeros(y.shape[1:], F32)

    @pl.when(gy == ny - 1)
    def _():
        for _b, y in bodies:
            y[1] = jnp.zeros(y.shape[1:], F32)

    W[ITERS - 1, lx + 1] = jnp.zeros((ly, zz), F32)

    if near:
        pl.semaphore_wait(barrier, ny + 1 - (gx == 0).astype(jnp.int32) - (gx == nx - 1).astype(jnp.int32))
    else:
        pl.semaphore_wait(barrier, nx + ny - 2)

    has = (gx > 0, gx < nx - 1, gy > 0, gy < ny - 1)
    to = (
        {"gx": jnp.maximum(gx - 1, 0)},
        {"gx": jnp.minimum(gx + 1, nx - 1)},
        {"gy": jnp.maximum(gy - 1, 0)},
        {"gy": jnp.minimum(gy + 1, ny - 1)},
    )

    def halo_copy(stage, d):
        body, y = bodies[stage]
        stag = stagings[stage]
        src, dst = (
            (body.at[1], body.at[lx + 1]),
            (body.at[lx], body.at[0]),
            (stag.at[0], y.at[1]),
            (stag.at[1], y.at[0]),
        )[d]
        return pltpu.make_async_remote_copy(
            src_ref=src, dst_ref=dst, send_sem=hs_sem.at[stage, d], recv_sem=hr_sem.at[stage, d],
            device_id=to[d], device_id_type=MESH,
        )

    one_way = ST_W + ITERS - 1

    def dirs(stage, among=(0, 1, 2, 3)):
        return [d for d in among if stage != one_way or d in (1, 3)]

    def send(stage, among=(0, 1, 2, 3)):
        for d in dirs(stage, among):
            @pl.when(has[d])
            def _():
                halo_copy(stage, d).start()

    def arrive(stage):
        for d in dirs(stage):
            @pl.when(has[d ^ 1])
            def _():
                halo_copy(stage, d).wait_recv()

    def sent(stage):
        for d in dirs(stage):
            @pl.when(has[d])
            def _():
                halo_copy(stage, d).wait_send()

    def gather(buf, axis, n, me, ss, rs):
        copies = []
        for p in range(1, n):
            cp = pltpu.make_async_remote_copy(
                src_ref=buf.at[0], dst_ref=buf.at[p], send_sem=ss.at[p], recv_sem=rs.at[p],
                device_id={axis: lax.rem(me + p, n)}, device_id_type=MESH,
            )
            cp.start()
            copies.append(cp)
        return copies

    def rows(fn, stage=None):
        def step(t, carry):
            fn(lax.rem(lx - t, lx))
            if stage is not None:
                @pl.when(t == min(1, lx - 1))
                def _():
                    send(stage, (0, 1))
            return carry
        lax.fori_loop(0, lx, step, 0)
        if stage is not None:
            send(stage, (2, 3))

    def stage_y(stage, i, x):
        stag = stagings[stage]
        stag[0, i] = x[0:1, :]
        stag[1, i] = x[ly - 1:ly, :]

    def sides(body, y, i):
        x = body[i + 1]
        z = x.shape[1]
        sub = lax.broadcasted_iota(jnp.int32, x.shape, 0)
        ym = jnp.where(sub == 0, y[0, i], pltpu.roll(x, 1, 0))
        yp = jnp.where(sub == ly - 1, y[1, i], pltpu.roll(x, ly - 1, 0))
        return x, body[i], body[i + 2], ym, yp, pltpu.roll(x, 1, 1), pltpu.roll(x, z - 1, 1)

    lane_g = lax.broadcasted_iota(jnp.int32, (ly, wg), 1)
    sub_g = lax.broadcasted_iota(jnp.int32, (ly, wg), 0)
    own_g = lane_g == gy * ly + sub_g
    lane_gf = lane_g.astype(F32)
    lane_t = lax.broadcasted_iota(jnp.int32, (ly, LANES), 1)
    lane_z = lax.broadcasted_iota(jnp.int32, (ly, zz), 1)

    loads["u"].wait()

    def take_low(i):
        x = U[0, i + 1, :, 0:LANES]
        Pb[0, i + 1] = x
        stage_y(ST_P, i, x)
    rows(take_low, ST_P)

    loads["v"].wait()

    def take_top(i):
        last = V[i + 1, :, zz - LANES:zz]
        TG[0, i] = jnp.sum(jnp.where(own_g, last[:, LANES - 1:LANES], 0.0), axis=0, keepdims=True)
        stage_y(ST_V, i, V[i + 1])
        stage_y(ST_U, i, U[0, i + 1])
    rows(take_top)
    tops = gather(TG, "gy", ny, gy, tg_s, tg_r)

    loads["k"].wait()

    def take_k(i):
        stage_y(ST_K, i, K[i + 1])
    rows(take_k, ST_K)
    send(ST_V)

    loads["map"].wait()
    loads["flags"].wait()
    loads["d"].wait()
    loads["c"].wait()
    eye = lax.broadcasted_iota(jnp.int32, (ly, ly), 0) == lax.broadcasted_iota(jnp.int32, (ly, ly), 1)
    for i in range(lx):
        line = MAP[i:i + 1, :].astype(F32)
        lk = jnp.sum(jnp.where(eye, line, 0.0), axis=1, keepdims=True)
        LK[i] = jnp.broadcast_to(lk, (ly, LANES))

    def fluid_coefficients(i):
        for t in range(zz // ZB):
            sl = pl.ds(t * ZB, ZB)
            line = FLAGS[i, t:t + 1, :].astype(F32)
            on = jnp.broadcast_to(jnp.sum(jnp.where(eye, line, 0.0), axis=1, keepdims=True), (ly, ZB))
            spread = on * D[i, :, sl]
            total = None
            for comp, (lo, hi) in enumerate(((CXm, CXp), (CYm, CYp), (CZm, CZp))):
                flow = on * C[comp, i, :, sl]
                a = spread + jnp.maximum(flow, 0.0)
                b = spread - jnp.minimum(flow, 0.0)
                total = a + b if total is None else total + (a + b)
                if comp == 2 and t == 0:
                    lane = lax.broadcasted_iota(jnp.int32, (ly, ZB), 1)
                    Q[i] = jnp.where(lane == 0, a, 0.0)[:, 0:LANES]
                    a = jnp.where(lane == 0, 0.0, a)
                if comp == 2 and t == zz // ZB - 1:
                    lane = lax.broadcasted_iota(jnp.int32, (ly, ZB), 1)
                    b = jnp.where(lane == ZB - 1, 0.0, b)
                lo[i, :, sl] = a
                hi[i, :, sl] = b
            CC[i, :, sl] = 1.0 - total
    rows(fluid_coefficients)

    for cp in tops:
        cp.wait_recv()

    def ghosts(i):
        whole = TG[0, i]
        for p in range(1, ny):
            whole = whole + TG[p, i]
        pick = jnp.where(lane_gf == LK[i, :, 0:1], whole, 0.0)
        ghost = jnp.sum(pick, axis=1, keepdims=True)
        GH[i] = jnp.broadcast_to(ghost, (ly, LANES))
        Q[i] = Q[i] * ghost
        FS[i] = Pb[0, i + 1] - ghost
    rows(ghosts)

    def fluid(body, y, i, z):
        x, a, b, c, d, e, f = sides(body, y, i)
        sl = pl.ds(0, z)
        return (CC[i, :, sl] * x + CXm[i, :, sl] * a + CXp[i, :, sl] * b + CYm[i, :, sl] * c
                + CYp[i, :, sl] * d + CZm[i, :, sl] * e + CZp[i, :, sl] * f)

    for s in range(SUBSTEPS - 1):
        arrive(ST_P + s)

        def low(i):
            new = fluid(Pb.at[s], yP.at[s], i, LANES) + Q[i]
            FS[i] = FS[i] + (new - GH[i])
            if s + 1 < SUBSTEPS - 1:
                Pb[s + 1, i + 1] = new
                stage_y(ST_P + s + 1, i, new)
        rows(low, ST_P + s + 1 if s + 1 < SUBSTEPS - 1 else None)
        if s == 1:
            send(ST_U)

    def scatter(i):
        mean = FS[i][:, 0:1] * (1.0 / SUBSTEPS)
        AG[0, i] = jnp.sum(jnp.where(lane_gf == LK[i, :, 0:1], mean, 0.0), axis=0, keepdims=True)
    rows(scatter)
    fluxes = gather(AG, "gy", ny, gy, ag_s, ag_r)

    arrive(ST_K)
    loads["cap"].wait()
    loads["heat"].wait()
    for f in range(lx + 1):
        GX[f] = 0.5 * (K[f] + K[f + 1])

    def solid_coefficients(i):
        k, _a, _b, c, d, e, f = sides(K, yK, i)
        gxm, gxp, gym, gyp = GX[i], GX[i + 1], 0.5 * (k + c), 0.5 * (k + d)
        gzm = 0.5 * (k + jnp.where(lane_z == 0, 0.0, e))
        gzp = 0.5 * (k + jnp.where(lane_z == zz - 1, 0.0, f))
        diag = CAP[i] + (gxm + gxp + gym + gyp + gzm + gzp)
        DI[i] = diag
        INV[i] = 1.0 / diag
        GYm[i] = gym
        GYp[i] = gyp
        GZm[i] = jnp.where(lane_z == 0, 0.0, gzm)
        GZp[i] = jnp.where(lane_z == zz - 1, 0.0, gzp)
    rows(solid_coefficients)

    def pull(body, y, i):
        x, a, b, c, d, e, f = sides(body, y, i)
        return x, (GX[i] * a + GX[i + 1] * b + GYm[i] * c + GYp[i] * d + GZm[i] * e + GZp[i] * f)

    arrive(ST_V)

    def first(i):
        x, s = pull(V, yV, i)
        W[0, i + 1] = (HEAT[i] - (DI[i] - CAP[i]) * x + s) * INV[i]
    rows(first)

    for cp in fluxes:
        cp.wait_recv()

    def fold(x):
        acc = x[0:8, 0:LANES]
        for r in range(0, ly, 8):
            for t in range(0, zz, LANES):
                if r or t:
                    acc = acc + x[r:r + 8, t:t + LANES]
        return jnp.sum(acc, axis=0, keepdims=True)

    def add_flux(i):
        whole = AG[0, i]
        for p in range(1, ny):
            whole = whole + AG[p, i]
        got = jnp.sum(jnp.where(own_g, whole, 0.0), axis=1, keepdims=True)
        sl = pl.ds(zz - LANES, LANES)
        W[0, i + 1, :, sl] = W[0, i + 1, :, sl] + jnp.where(lane_t == LANES - 1, got, 0.0) * INV[i, :, sl]
        stage_y(ST_W, i, W[0, i + 1])
    rows(add_flux, ST_W)

    MU[...] = jnp.zeros(MU.shape, F32)

    def norm(i):
        w = W[0, i + 1]
        MU[0:1] = MU[0:1] + fold(w * w * DI[i])
    rows(norm)

    def fluid_step(s):
        arrive(ST_U + s)
        last_u = s + 1 == SUBSTEPS

        def bulk(i):
            new = fluid(U.at[s], yU.at[s], i, zz)
            head = new[:, 0:LANES] + Q[i]
            if last_u:
                UO[i] = new
                UO[i, :, 0:LANES] = head
            else:
                U[s + 1, i + 1] = new
                U[s + 1, i + 1, :, 0:LANES] = head
                stage_y(ST_U + s + 1, i, U[s + 1, i + 1])
        rows(bulk, None if last_u else ST_U + s + 1)

    def solid_step(s):
        arrive(ST_W + s)

        def apply(i):
            x, pulled = pull(W.at[s], yW.at[s], i)
            MU[2 * s + 1:2 * s + 2] = MU[2 * s + 1:2 * s + 2] + fold(x * pulled)
            new = pulled * INV[i]
            W[s + 1, i + 1] = new
            stage_y(ST_W + s + 1, i, new)
            MU[2 * s + 2:2 * s + 3] = MU[2 * s + 2:2 * s + 3] + fold(new * pulled)
        rows(apply, ST_W + s + 1)

    for s in range(max(SUBSTEPS, ITERS) - 1):
        if s < ITERS - 1:
            solid_step(s)
        if s < SUBSTEPS - 1:
            fluid_step(s)

    arrive(one_way)
    end = ITERS - 1

    def last_moment(i):
        x = W[end, i + 1]
        z = x.shape[1]
        sub = lax.broadcasted_iota(jnp.int32, x.shape, 0)
        twice = jnp.where(i == 0, 2.0, 1.0).astype(F32)
        ym = jnp.where(sub == 0, 2.0 * yW[end, 0, i], pltpu.roll(x, 1, 0))
        yp = jnp.where(sub == ly - 1, 0.0, pltpu.roll(x, ly - 1, 0))
        pulled = (GX[i] * (twice * W[end, i]) + GX[i + 1] * W[end, i + 2] + GYm[i] * ym + GYp[i] * yp
                  + GZm[i] * pltpu.roll(x, 1, 1) + GZp[i] * pltpu.roll(x, z - 1, 1))
        MU[2 * end + 1:2 * end + 2] = MU[2 * end + 1:2 * end + 2] + fold(x * pulled)
    rows(last_moment)

    MGY[0] = MU[...]
    sums_y = gather(MGY, "gy", ny, gy, my_s, my_r)
    for cp in sums_y:
        cp.wait_recv()
    total = MGY[0]
    for p in range(1, ny):
        total = total + MGY[p]
    MGX[0] = jnp.broadcast_to(jnp.sum(total, axis=1, keepdims=True), total.shape)
    sums_x = gather(MGX, "gx", nx, gx, mx_s, mx_r)
    fluid_step(SUBSTEPS - 1)
    out_u = pltpu.make_async_copy(UO, u_out, out_sem.at[0])
    out_u.start()
    for cp in sums_x:
        cp.wait_recv()
    total = MGX[0]
    for p in range(1, nx):
        total = total + MGX[p]
    mu = [total[m:m + 1, :] for m in range(2 * ITERS)]

    tiny = 1e-30
    G = [[mu[i + j] - mu[i + j + 1] for j in range(ITERS)] for i in range(ITERS)]
    b = [mu[i] for i in range(ITERS)]
    low_f = {}
    rec = []
    for i in range(ITERS):
        good = G[i][i] > jnp.maximum(1e-7 * (mu[2 * i] + jnp.abs(mu[2 * i + 1])), tiny)
        r = jnp.where(good, 1.0 / jnp.where(good, G[i][i], 1.0), 0.0)
        rec.append(r)
        for j in range(i + 1, ITERS):
            low_f[j, i] = G[j][i] * r
        for j in range(i + 1, ITERS):
            b[j] = b[j] - low_f[j, i] * b[i]
            for m in range(i + 1, ITERS):
                G[j][m] = G[j][m] - low_f[j, i] * G[i][m]
    y = [None] * ITERS
    for i in reversed(range(ITERS)):
        y[i] = b[i] * rec[i]
        for j in range(i + 1, ITERS):
            y[i] = y[i] - low_f[j, i] * y[j]

    ys = [v[:, 0:1] for v in y]

    def finish(i):
        acc = V[i + 1]
        for j in range(ITERS):
            acc = acc + ys[j] * W[j, i + 1]
        VO[i] = acc
    rows(finish)
    out_v = pltpu.make_async_copy(VO, v_out, out_sem.at[1])
    out_v.start()

    for stage in range(STAGES):
        sent(stage)
    for cp in tops + fluxes + sums_y + sums_x:
        cp.wait_send()
    out_u.wait()
    out_v.wait()


def solution(mesh):
    nx, ny = mesh.shape["gx"], mesh.shape["gy"]

    def local(u, d, c, flags, v, cap, k, heat, lookup):
        lx, ly, zz = u.shape
        wg = -(-(ny * ly) // LANES) * LANES
        field = (lx, ly, zz)
        padded = (lx + 2, ly, zz)
        edge = (2, lx, 1, zz)
        low = (2, lx, 1, LANES)
        tile = (lx, ly, LANES)
        vm = lambda *shape: pltpu.VMEM(shape, F32)
        ns = SUBSTEPS
        scratch = [
            vm(ns, *padded), vm(ns - 1, lx + 2, ly, LANES), vm(*padded), vm(*padded), vm(ITERS, *padded),
            vm(ns, *edge), vm(ns - 1, *low), vm(*edge), vm(*edge), vm(ITERS, *edge),
            vm(ns, *edge), vm(ns - 1, *low), vm(*edge), vm(*edge), vm(ITERS, *edge),
            vm(*field), vm(3, *field), pltpu.VMEM((lx, flags.shape[2], ly), jnp.int32), vm(*field), vm(*field),
            pltpu.VMEM(lookup.shape, jnp.int32),
        ]
        scratch += [vm(*field)] * 7 + [vm(*tile)] * 4
        scratch += [vm(lx + 1, ly, zz)] + [vm(*field)] * 6
        scratch += [
            vm(ny, lx, 1, wg), vm(ny, lx, 1, wg), vm(2 * ITERS, LANES), vm(ny, 2 * ITERS, LANES),
            vm(2 * ITERS, LANES), vm(nx, 2 * ITERS, LANES), vm(*field), vm(*field),
        ]
        dma = lambda *shape: pltpu.SemaphoreType.DMA(shape)
        scratch += [
            dma(9), dma(2), dma(STAGES, 4), dma(STAGES, 4),
            dma(ny), dma(ny), dma(ny), dma(ny), dma(ny), dma(ny), dma(nx), dma(nx),
        ]
        return pl.pallas_call(
            functools.partial(kernel, nx, ny),
            out_shape=(jax.ShapeDtypeStruct(field, F32),) * 2,
            in_specs=[pl.BlockSpec(memory_space=pltpu.HBM)] * 9,
            out_specs=(pl.BlockSpec(memory_space=pl.ANY),) * 2,
            scratch_shapes=scratch,
            compiler_params=pltpu.CompilerParams(
                collective_id=0, has_side_effects=True, vmem_limit_bytes=67_000_000
            ),
        )(u, d, c, jnp.swapaxes(flags, 1, 2), v, cap, k, heat, lookup)

    s3 = P("gx", "gy", None)
    return jax.shard_map(
        local,
        mesh=mesh,
        in_specs=(s3, s3, P(None, "gx", "gy", None), s3, s3, s3, s3, s3, P("gx", "gy")),
        out_specs=(s3, s3),
        check_vma=False,
    )
```

```python
import functools

import jax
import jax.numpy as jnp
from jax import lax
from jax.experimental import pallas as pl
from jax.experimental.pallas import tpu as pltpu
from jax.sharding import PartitionSpec as P

SUBSTEPS = 4
ITERS = 4
ZB = 128
LANES = 128
MESH = pl.DeviceIdType.MESH
F32 = jnp.float32

ST_P = 0
ST_U = ST_P + SUBSTEPS - 1
ST_K = ST_U + SUBSTEPS
ST_V = ST_K + 1
ST_W = ST_V + 1
STAGES = ST_W + ITERS
REACH = 1 + (SUBSTEPS - 1) + (ITERS - 1)


def kernel(
    nx, ny,
    u_hbm, d_hbm, c_hbm, flags_hbm, v_hbm, cap_hbm, k_hbm, heat_hbm, map_hbm,
    UO, VO,
    U, Pb, K, V, W,
    yU, yP, yK, yV, yW,
    sU, sP, sK, sV, sW,
    D, C, FLAGS, CAP, HEAT, MAP,
    CC, CXm, CXp, CYm, CYp, CZm, CZp, Q, GH, LK, FS,
    GX, GYm, GYp, GZm, GZp, DI, INV,
    TG, AG, MU, MGY, MSX, MGX,
    in_sem, hs_sem, hr_sem, tg_s, tg_r, ag_s, ag_r, my_s, my_r, mx_s, mx_r,
):
    gx = lax.axis_index("gx")
    gy = lax.axis_index("gy")
    lx, ly, zz = CAP.shape
    wg = TG.shape[-1]

    loads = {}

    def load(name, src, dst, n):
        cp = pltpu.make_async_copy(src, dst, in_sem.at[n])
        cp.start()
        loads[name] = cp

    load("u", u_hbm, U.at[0, pl.ds(1, lx)], 0)
    load("v", v_hbm, V.at[pl.ds(1, lx)], 1)
    load("k", k_hbm, K.at[pl.ds(1, lx)], 2)
    load("map", map_hbm, MAP, 3)
    load("flags", flags_hbm, FLAGS, 4)
    load("d", d_hbm, D, 5)
    load("c", c_hbm, C, 6)
    load("heat", heat_hbm, HEAT, 7)
    load("cap", cap_hbm, CAP, 8)

    barrier = pltpu.get_barrier_semaphore()
    near = nx - 1 <= REACH
    if near:
        @pl.when(gx > 0)
        def _():
            pl.semaphore_signal(barrier, 1, device_id={"gx": jnp.maximum(gx - 1, 0)}, device_id_type=MESH)

        @pl.when(gx < nx - 1)
        def _():
            pl.semaphore_signal(barrier, 1, device_id={"gx": jnp.minimum(gx + 1, nx - 1)}, device_id_type=MESH)
    else:
        for p in range(1, nx):
            pl.semaphore_signal(barrier, 1, device_id={"gx": lax.rem(gx + p, nx)}, device_id_type=MESH)
    for p in range(1, ny):
        pl.semaphore_signal(barrier, 1, device_id={"gy": lax.rem(gy + p, ny)}, device_id_type=MESH)

    bodies = (
        [(Pb.at[s], yP.at[s]) for s in range(SUBSTEPS - 1)]
        + [(U.at[s], yU.at[s]) for s in range(SUBSTEPS)]
        + [(K, yK), (V, yV)]
        + [(W.at[s], yW.at[s]) for s in range(ITERS)]
    )
    stagings = (
        [sP.at[s] for s in range(SUBSTEPS - 1)]
        + [sU.at[s] for s in range(SUBSTEPS)]
        + [sK, sV]
        + [sW.at[s] for s in range(ITERS)]
    )

    @pl.when(gx == 0)
    def _():
        for body, _y in bodies:
            body[0] = jnp.zeros(body.shape[1:], F32)

    @pl.when(gx == nx - 1)
    def _():
        for body, _y in bodies:
            body[lx + 1] = jnp.zeros(body.shape[1:], F32)

    @pl.when(gy == 0)
    def _():
        for _b, y in bodies:
            y[0] = jnp.zeros(y.shape[1:], F32)

    @pl.when(gy == ny - 1)
    def _():
        for _b, y in bodies:
            y[1] = jnp.zeros(y.shape[1:], F32)

    W[ITERS - 1, lx + 1] = jnp.zeros((ly, zz), F32)

    if near:
        pl.semaphore_wait(barrier, ny + 1 - (gx == 0).astype(jnp.int32) - (gx == nx - 1).astype(jnp.int32))
    else:
        pl.semaphore_wait(barrier, nx + ny - 2)

    has = (gx > 0, gx < nx - 1, gy > 0, gy < ny - 1)
    to = (
        {"gx": jnp.maximum(gx - 1, 0)},
        {"gx": jnp.minimum(gx + 1, nx - 1)},
        {"gy": jnp.maximum(gy - 1, 0)},
        {"gy": jnp.minimum(gy + 1, ny - 1)},
    )

    def halo_copy(stage, d):
        body, y = bodies[stage]
        stag = stagings[stage]
        src, dst = (
            (body.at[1], body.at[lx + 1]),
            (body.at[lx], body.at[0]),
            (stag.at[0], y.at[1]),
            (stag.at[1], y.at[0]),
        )[d]
        return pltpu.make_async_remote_copy(
            src_ref=src, dst_ref=dst, send_sem=hs_sem.at[stage, d], recv_sem=hr_sem.at[stage, d],
            device_id=to[d], device_id_type=MESH,
        )

    one_way = ST_W + ITERS - 1

    def dirs(stage, among=(0, 1, 2, 3)):
        return [d for d in among if stage != one_way or d in (1, 3)]

    def send(stage, among=(0, 1, 2, 3)):
        for d in dirs(stage, among):
            @pl.when(has[d])
            def _():
                halo_copy(stage, d).start()

    def arrive(stage):
        for d in dirs(stage):
            @pl.when(has[d ^ 1])
            def _():
                halo_copy(stage, d).wait_recv()

    def sent(stage):
        for d in dirs(stage):
            @pl.when(has[d])
            def _():
                halo_copy(stage, d).wait_send()

    def gather(buf, axis, n, me, ss, rs):
        copies = []
        for p in range(1, n):
            cp = pltpu.make_async_remote_copy(
                src_ref=buf.at[0], dst_ref=buf.at[p], send_sem=ss.at[p], recv_sem=rs.at[p],
                device_id={axis: lax.rem(me + p, n)}, device_id_type=MESH,
            )
            cp.start()
            copies.append(cp)
        return copies

    def rows(fn, stage=None):
        def step(t, carry):
            fn(lax.rem(lx - t, lx))
            if stage is not None:
                @pl.when(t == min(1, lx - 1))
                def _():
                    send(stage, (0, 1))
            return carry
        lax.fori_loop(0, lx, step, 0)
        if stage is not None:
            send(stage, (2, 3))

    def stage_y(stage, i, x):
        stag = stagings[stage]
        stag[0, i] = x[0:1, :]
        stag[1, i] = x[ly - 1:ly, :]

    def sides(body, y, i):
        x = body[i + 1]
        z = x.shape[1]
        sub = lax.broadcasted_iota(jnp.int32, x.shape, 0)
        ym = jnp.where(sub == 0, y[0, i], pltpu.roll(x, 1, 0))
        yp = jnp.where(sub == ly - 1, y[1, i], pltpu.roll(x, ly - 1, 0))
        return x, body[i], body[i + 2], ym, yp, pltpu.roll(x, 1, 1), pltpu.roll(x, z - 1, 1)

    lane_g = lax.broadcasted_iota(jnp.int32, (ly, wg), 1)
    sub_g = lax.broadcasted_iota(jnp.int32, (ly, wg), 0)
    own_g = lane_g == gy * ly + sub_g
    lane_gf = lane_g.astype(F32)
    lane_t = lax.broadcasted_iota(jnp.int32, (ly, LANES), 1)
    lane_z = lax.broadcasted_iota(jnp.int32, (ly, zz), 1)

    loads["u"].wait()

    def take_low(i):
        x = U[0, i + 1, :, 0:LANES]
        Pb[0, i + 1] = x
        stage_y(ST_P, i, x)
    rows(take_low, ST_P)

    loads["v"].wait()

    def take_top(i):
        last = V[i + 1, :, zz - LANES:zz]
        TG[0, i] = jnp.sum(jnp.where(own_g, last[:, LANES - 1:LANES], 0.0), axis=0, keepdims=True)
        stage_y(ST_V, i, V[i + 1])
        stage_y(ST_U, i, U[0, i + 1])
    rows(take_top)
    tops = gather(TG, "gy", ny, gy, tg_s, tg_r)

    loads["k"].wait()

    def take_k(i):
        stage_y(ST_K, i, K[i + 1])
    rows(take_k, ST_K)
    send(ST_V)

    loads["map"].wait()
    loads["flags"].wait()
    loads["d"].wait()
    loads["c"].wait()
    eye = lax.broadcasted_iota(jnp.int32, (ly, ly), 0) == lax.broadcasted_iota(jnp.int32, (ly, ly), 1)
    for i in range(lx):
        line = MAP[i:i + 1, :].astype(F32)
        lk = jnp.sum(jnp.where(eye, line, 0.0), axis=1, keepdims=True)
        LK[i] = jnp.broadcast_to(lk, (ly, LANES))

    def fluid_coefficients(i):
        for t in range(zz // ZB):
            sl = pl.ds(t * ZB, ZB)
            line = FLAGS[i, t:t + 1, :].astype(F32)
            on = jnp.broadcast_to(jnp.sum(jnp.where(eye, line, 0.0), axis=1, keepdims=True), (ly, ZB))
            spread = on * D[i, :, sl]
            total = None
            for comp, (lo, hi) in enumerate(((CXm, CXp), (CYm, CYp), (CZm, CZp))):
                flow = on * C[comp, i, :, sl]
                a = spread + jnp.maximum(flow, 0.0)
                b = spread - jnp.minimum(flow, 0.0)
                total = a + b if total is None else total + (a + b)
                if comp == 2 and t == 0:
                    lane = lax.broadcasted_iota(jnp.int32, (ly, ZB), 1)
                    Q[i] = jnp.where(lane == 0, a, 0.0)[:, 0:LANES]
                    a = jnp.where(lane == 0, 0.0, a)
                if comp == 2 and t == zz // ZB - 1:
                    lane = lax.broadcasted_iota(jnp.int32, (ly, ZB), 1)
                    b = jnp.where(lane == ZB - 1, 0.0, b)
                lo[i, :, sl] = a
                hi[i, :, sl] = b
            CC[i, :, sl] = 1.0 - total
    rows(fluid_coefficients)

    for cp in tops:
        cp.wait_recv()

    def ghosts(i):
        whole = TG[0, i]
        for p in range(1, ny):
            whole = whole + TG[p, i]
        pick = jnp.where(lane_gf == LK[i, :, 0:1], whole, 0.0)
        ghost = jnp.sum(pick, axis=1, keepdims=True)
        GH[i] = jnp.broadcast_to(ghost, (ly, LANES))
        Q[i] = Q[i] * ghost
        FS[i] = Pb[0, i + 1] - ghost
    rows(ghosts)

    def fluid(body, y, i, z):
        x, a, b, c, d, e, f = sides(body, y, i)
        sl = pl.ds(0, z)
        return (CC[i, :, sl] * x + CXm[i, :, sl] * a + CXp[i, :, sl] * b + CYm[i, :, sl] * c
                + CYp[i, :, sl] * d + CZm[i, :, sl] * e + CZp[i, :, sl] * f)

    for s in range(SUBSTEPS - 1):
        arrive(ST_P + s)

        def low(i):
            new = fluid(Pb.at[s], yP.at[s], i, LANES) + Q[i]
            FS[i] = FS[i] + (new - GH[i])
            if s + 1 < SUBSTEPS - 1:
                Pb[s + 1, i + 1] = new
                stage_y(ST_P + s + 1, i, new)
        rows(low, ST_P + s + 1 if s + 1 < SUBSTEPS - 1 else None)
        if s == 1:
            send(ST_U)

    def scatter(i):
        mean = FS[i][:, 0:1] * (1.0 / SUBSTEPS)
        AG[0, i] = jnp.sum(jnp.where(lane_gf == LK[i, :, 0:1], mean, 0.0), axis=0, keepdims=True)
    rows(scatter)
    fluxes = gather(AG, "gy", ny, gy, ag_s, ag_r)

    arrive(ST_K)
    loads["cap"].wait()
    loads["heat"].wait()
    for f in range(lx + 1):
        GX[f] = 0.5 * (K[f] + K[f + 1])

    def solid_coefficients(i):
        k, _a, _b, c, d, e, f = sides(K, yK, i)
        gxm, gxp, gym, gyp = GX[i], GX[i + 1], 0.5 * (k + c), 0.5 * (k + d)
        gzm = 0.5 * (k + jnp.where(lane_z == 0, 0.0, e))
        gzp = 0.5 * (k + jnp.where(lane_z == zz - 1, 0.0, f))
        diag = CAP[i] + (gxm + gxp + gym + gyp + gzm + gzp)
        DI[i] = diag
        INV[i] = 1.0 / diag
        GYm[i] = gym
        GYp[i] = gyp
        GZm[i] = jnp.where(lane_z == 0, 0.0, gzm)
        GZp[i] = jnp.where(lane_z == zz - 1, 0.0, gzp)
    rows(solid_coefficients)

    def pull(body, y, i):
        x, a, b, c, d, e, f = sides(body, y, i)
        return x, (GX[i] * a + GX[i + 1] * b + GYm[i] * c + GYp[i] * d + GZm[i] * e + GZp[i] * f)

    arrive(ST_V)

    def first(i):
        x, s = pull(V, yV, i)
        W[0, i + 1] = (HEAT[i] - (DI[i] - CAP[i]) * x + s) * INV[i]
    rows(first)

    for cp in fluxes:
        cp.wait_recv()

    def fold(x):
        acc = x[0:8, 0:LANES]
        for r in range(0, ly, 8):
            for t in range(0, zz, LANES):
                if r or t:
                    acc = acc + x[r:r + 8, t:t + LANES]
        return jnp.sum(acc, axis=0, keepdims=True)

    def add_flux(i):
        whole = AG[0, i]
        for p in range(1, ny):
            whole = whole + AG[p, i]
        got = jnp.sum(jnp.where(own_g, whole, 0.0), axis=1, keepdims=True)
        sl = pl.ds(zz - LANES, LANES)
        W[0, i + 1, :, sl] = W[0, i + 1, :, sl] + jnp.where(lane_t == LANES - 1, got, 0.0) * INV[i, :, sl]
        stage_y(ST_W, i, W[0, i + 1])
    rows(add_flux, ST_W)

    MU[...] = jnp.zeros(MU.shape, F32)

    def norm(i):
        w = W[0, i + 1]
        MU[0:1] = MU[0:1] + fold(w * w * DI[i])
    rows(norm)

    def fluid_step(s):
        arrive(ST_U + s)
        last_u = s + 1 == SUBSTEPS

        def bulk(i):
            new = fluid(U.at[s], yU.at[s], i, zz)
            head = new[:, 0:LANES] + Q[i]
            if last_u:
                UO[i] = new
                UO[i, :, 0:LANES] = head
            else:
                U[s + 1, i + 1] = new
                U[s + 1, i + 1, :, 0:LANES] = head
                stage_y(ST_U + s + 1, i, U[s + 1, i + 1])
        rows(bulk, None if last_u else ST_U + s + 1)

    def solid_step(s):
        arrive(ST_W + s)

        def apply(i):
            x, pulled = pull(W.at[s], yW.at[s], i)
            MU[2 * s + 1:2 * s + 2] = MU[2 * s + 1:2 * s + 2] + fold(x * pulled)
            new = pulled * INV[i]
            W[s + 1, i + 1] = new
            stage_y(ST_W + s + 1, i, new)
            MU[2 * s + 2:2 * s + 3] = MU[2 * s + 2:2 * s + 3] + fold(new * pulled)
        rows(apply, ST_W + s + 1)

    for s in range(max(SUBSTEPS, ITERS) - 1):
        if s < ITERS - 1:
            solid_step(s)
        if s < SUBSTEPS - 1:
            fluid_step(s)

    arrive(one_way)
    end = ITERS - 1

    def last_moment(i):
        x = W[end, i + 1]
        z = x.shape[1]
        sub = lax.broadcasted_iota(jnp.int32, x.shape, 0)
        twice = jnp.where(i == 0, 2.0, 1.0).astype(F32)
        ym = jnp.where(sub == 0, 2.0 * yW[end, 0, i], pltpu.roll(x, 1, 0))
        yp = jnp.where(sub == ly - 1, 0.0, pltpu.roll(x, ly - 1, 0))
        pulled = (GX[i] * (twice * W[end, i]) + GX[i + 1] * W[end, i + 2] + GYm[i] * ym + GYp[i] * yp
                  + GZm[i] * pltpu.roll(x, 1, 1) + GZp[i] * pltpu.roll(x, z - 1, 1))
        MU[2 * end + 1:2 * end + 2] = MU[2 * end + 1:2 * end + 2] + fold(x * pulled)
    rows(last_moment)

    MGY[0] = MU[...]
    sums_y = gather(MGY, "gy", ny, gy, my_s, my_r)
    for cp in sums_y:
        cp.wait_recv()
    total = MGY[0]
    for p in range(1, ny):
        total = total + MGY[p]
    MGX[0] = jnp.broadcast_to(jnp.sum(total, axis=1, keepdims=True), total.shape)
    sums_x = gather(MGX, "gx", nx, gx, mx_s, mx_r)
    fluid_step(SUBSTEPS - 1)
    for cp in sums_x:
        cp.wait_recv()
    total = MGX[0]
    for p in range(1, nx):
        total = total + MGX[p]
    mu = [total[m:m + 1, :] for m in range(2 * ITERS)]

    tiny = 1e-30
    G = [[mu[i + j] - mu[i + j + 1] for j in range(ITERS)] for i in range(ITERS)]
    b = [mu[i] for i in range(ITERS)]
    low_f = {}
    rec = []
    for i in range(ITERS):
        good = G[i][i] > jnp.maximum(1e-7 * (mu[2 * i] + jnp.abs(mu[2 * i + 1])), tiny)
        r = jnp.where(good, 1.0 / jnp.where(good, G[i][i], 1.0), 0.0)
        rec.append(r)
        for j in range(i + 1, ITERS):
            low_f[j, i] = G[j][i] * r
        for j in range(i + 1, ITERS):
            b[j] = b[j] - low_f[j, i] * b[i]
            for m in range(i + 1, ITERS):
                G[j][m] = G[j][m] - low_f[j, i] * G[i][m]
    y = [None] * ITERS
    for i in reversed(range(ITERS)):
        y[i] = b[i] * rec[i]
        for j in range(i + 1, ITERS):
            y[i] = y[i] - low_f[j, i] * y[j]

    ys = [v[:, 0:1] for v in y]

    def finish(i):
        acc = V[i + 1]
        for j in range(ITERS):
            acc = acc + ys[j] * W[j, i + 1]
        VO[i] = acc
    rows(finish)

    for stage in range(STAGES):
        sent(stage)
    for cp in tops + fluxes + sums_y + sums_x:
        cp.wait_send()


def solution(mesh):
    nx, ny = mesh.shape["gx"], mesh.shape["gy"]

    def local(u, d, c, flags, v, cap, k, heat, lookup):
        lx, ly, zz = u.shape
        wg = -(-(ny * ly) // LANES) * LANES
        field = (lx, ly, zz)
        padded = (lx + 2, ly, zz)
        edge = (2, lx, 1, zz)
        low = (2, lx, 1, LANES)
        tile = (lx, ly, LANES)
        vm = lambda *shape: pltpu.VMEM(shape, F32)
        ns = SUBSTEPS
        scratch = [
            vm(ns, *padded), vm(ns - 1, lx + 2, ly, LANES), vm(*padded), vm(*padded), vm(ITERS, *padded),
            vm(ns, *edge), vm(ns - 1, *low), vm(*edge), vm(*edge), vm(ITERS, *edge),
            vm(ns, *edge), vm(ns - 1, *low), vm(*edge), vm(*edge), vm(ITERS, *edge),
            vm(*field), vm(3, *field), pltpu.VMEM((lx, flags.shape[2], ly), jnp.int32), vm(*field), vm(*field),
            pltpu.VMEM(lookup.shape, jnp.int32),
        ]
        scratch += [vm(*field)] * 7 + [vm(*tile)] * 4
        scratch += [vm(lx + 1, ly, zz)] + [vm(*field)] * 6
        scratch += [
            vm(ny, lx, 1, wg), vm(ny, lx, 1, wg), vm(2 * ITERS, LANES), vm(ny, 2 * ITERS, LANES),
            vm(2 * ITERS, LANES), vm(nx, 2 * ITERS, LANES),
        ]
        dma = lambda *shape: pltpu.SemaphoreType.DMA(shape)
        scratch += [
            dma(9), dma(STAGES, 4), dma(STAGES, 4),
            dma(ny), dma(ny), dma(ny), dma(ny), dma(ny), dma(ny), dma(nx), dma(nx),
        ]
        return pl.pallas_call(
            functools.partial(kernel, nx, ny),
            out_shape=(pltpu.VMEM(field, F32),) * 2,
            in_specs=[pl.BlockSpec(memory_space=pltpu.HBM)] * 9,
            out_specs=(pl.BlockSpec(memory_space=pltpu.VMEM),) * 2,
            scratch_shapes=scratch,
            compiler_params=pltpu.CompilerParams(
                collective_id=0, has_side_effects=True, vmem_limit_bytes=65000000
            ),
        )(u, d, c, jnp.swapaxes(flags, 1, 2), v, cap, k, heat, lookup)

    s3 = P("gx", "gy", None)
    return jax.shard_map(
        local,
        mesh=mesh,
        in_specs=(s3, s3, P(None, "gx", "gy", None), s3, s3, s3, s3, s3, P("gx", "gy")),
        out_specs=(s3, s3),
        check_vma=False,
    )
```
